32 devices in a mesh: dp: 8 (over z, x), tensor: 4 (over y, core).
Axes of the slice: x: 2, y: 2, z: 4, core: 2. Of those that a mesh axis runs over, the one named last changes fastest.
Arguments:
- attn_out: bfloat16 [4096, 2560], P('dp', 'tensor'), may hold values from -6 to 6
- resid: bfloat16 [4096, 5120], P('dp', 'tensor'), may hold values from -6 to 6
- out_proj: bfloat16 [2560, 5120], P('tensor'), may hold values from -0.125 to 0.125
- heads: bfloat16 [5120, 8], P('tensor'), may hold values from -0.078125 to 0.078125
- gain: bfloat16 [5120], P('tensor'), may hold values from 0.25 to 1.75
- lengths: int32 [64], P('dp'), may hold values from 0 to 63
Outputs:
- uwo: float32 [64], P('dp')
- proj_grad: float32 [5120, 2560], P('dp', 'tensor')
- head_grad: float32 [5120, 8], P('tensor')
- gain_grad: float32 [5120], P('tensor')
The draws below stay inside these ranges and needn't reach their ends.
Inputs may be any that keep to these rules, and one draw needn't show every extreme that they name: Positions 0 to lengths[n] of response n are scored.
All inputs are finite; a program needn't handle non-finite values.
Results may differ from the reference program's by a relative error of at most 0.0085.
Values may be sent and summed in bfloat16 or wider, within the bound.
A program may use at most 128 MiB of HBM per device.

```python
import jax
import jax.numpy as jnp
from jax import lax

D = 5120
HIN = 2560
HEADS = 8
RESP_DEV = 8
SEQ = 64
RESPONSES = 64
N_DP = 8
N_TENSOR = 4


def plant(entries, own_key, low, high):
    longest = entries.shape.index(max(entries.shape))
    spots = []
    for shift in (0, 1):
        where = [jax.random.randint(jax.random.fold_in(own_key, axis), (), 0, length) for axis, length in enumerate(entries.shape)]
        where[longest] = (where[longest] + shift) % entries.shape[longest]
        spots.append(tuple(where))
    return entries.at[spots[0]].set(low).at[spots[1]].set(high)


def block_scale(stream_key, dims, shards, low, high):
    level = 1.0
    for axis_at, parts in shards:
        heights = jax.random.uniform(jax.random.fold_in(jax.random.fold_in(stream_key, 6), axis_at), (parts,), jnp.float32, low / len(shards), high / len(shards))
        level = level * jnp.repeat(jnp.exp(heights), dims[axis_at] // parts).reshape((-1,) + (1,) * (len(dims) - 1 - axis_at))
    return level


def noise(rng, shape, scale, limit, cuts=(), kind=jnp.bfloat16):
    values = scale * jax.random.normal(rng, shape, jnp.float32)
    if cuts:
        values = values * block_scale(rng, shape, cuts, -0.22, 0.18)
    return jnp.clip(values, -limit, limit).astype(kind)


def setup_inputs(seed: int = 0) -> dict:
    seeds = jax.random.split(jax.random.key(seed), 7)
    attn_out = noise(seeds[0], (RESPONSES * SEQ, HIN), 1.0, 6.0, ((0, 8), (1, 4)))
    resid = noise(seeds[1], (RESPONSES * SEQ, D), 1.0, 6.0, ((0, 8), (1, 4)))
    out_proj = noise(seeds[2], (HIN, D), HIN ** -0.5, 0.125, ((0, 4),))
    heads = noise(seeds[3], (D, HEADS), D ** -0.5, 0.078125, ((0, 4),))
    gain = jnp.clip(1.0 + 0.15 * jax.random.normal(seeds[4], (D,), jnp.float32), 0.25, 1.75).astype(jnp.bfloat16)
    lengths = plant(jax.random.randint(seeds[5], (RESPONSES,), 0, SEQ), jax.random.fold_in(seeds[5], 1), 0, SEQ - 1).astype(jnp.int32)
    return {"attn_out": attn_out, "resid": resid, "out_proj": out_proj, "heads": heads, "gain": gain, "lengths": lengths}


EPS_NORM = 1e-06
EPS_VAR = 1e-05
PENALTY = 0.5

def hidden_rows(attn_block, resid_block, out_proj):
    width = attn_block.shape[1] // N_TENSOR
    total = resid_block.astype(jnp.float32)
    for block in range(N_TENSOR):
        product = jnp.dot(attn_block[:, block * width:(block + 1) * width], out_proj[block * width:(block + 1) * width], preferred_element_type=jnp.float32)
        total = total + lax.optimization_barrier(product.astype(jnp.bfloat16)).astype(jnp.float32)
    return total

def forward_block(attn_block, resid_block, out_proj, heads, gain):
    hidden = hidden_rows(attn_block, resid_block, out_proj)
    rinv = lax.rsqrt(lax.optimization_barrier(jnp.mean(hidden * hidden, axis=1)) + EPS_NORM)
    normed = hidden * rinv[:, None] * gain.astype(jnp.float32)[None, :]
    scores = jnp.dot(normed, heads.astype(jnp.float32), precision=lax.Precision.HIGHEST)
    return (hidden, rinv, normed, scores)

def masks(length_block):
    position = lax.broadcasted_iota(jnp.int32, (length_block.shape[0], SEQ), 1)
    inside = position <= length_block[:, None]
    counts = (length_block + 1).astype(jnp.float32)
    return (inside, counts)

def reference(attn_out, resid, out_proj, heads, gain, lengths):
    attn_blocks = attn_out.reshape(N_DP, RESP_DEV * SEQ, HIN)
    resid_blocks = resid.reshape(N_DP, RESP_DEV * SEQ, D)
    length_blocks = lengths.reshape(N_DP, RESP_DEV)

    def first_pass(items):
        attn_block, resid_block, length_block = items
        scores = forward_block(attn_block, resid_block, out_proj, heads, gain)[3]
        inside, counts = masks(length_block)
        per_resp = scores.reshape(RESP_DEV, SEQ, HEADS)
        summed = lax.optimization_barrier(jnp.sum(jnp.where(inside[:, :, None], per_resp, 0.0), axis=1))
        return summed / counts[:, None]
    rewards = lax.map(first_pass, (attn_blocks, resid_blocks, length_blocks)).reshape(RESPONSES, HEADS)
    center = lax.optimization_barrier(jnp.mean(rewards, axis=0))
    spread = lax.optimization_barrier(jnp.mean((rewards - center[None, :]) ** 2, axis=0))
    zed = (rewards - center[None, :]) * lax.rsqrt(spread + EPS_VAR)[None, :]
    zmean = lax.optimization_barrier(jnp.mean(zed, axis=1))
    uwo = zmean - PENALTY * lax.optimization_barrier(jnp.mean((zed - zmean[:, None]) ** 2, axis=1))
    pairs = rewards.reshape(RESPONSES // 2, 2, HEADS)
    weight = jax.nn.sigmoid(pairs[:, 1] - pairs[:, 0])
    dreward = jnp.stack([-weight, weight], axis=1).reshape(N_DP, RESP_DEV, HEADS)
    gain32 = gain.astype(jnp.float32)
    heads32 = heads.astype(jnp.float32)

    def second_pass(carry, items):
        proj_acc, head_acc, gain_acc = carry
        attn_block, resid_block, length_block, dreward_block = items
        hidden, rinv, normed, scores = forward_block(attn_block, resid_block, out_proj, heads, gain)
        inside, counts = masks(length_block)
        dscore = jnp.where(inside[:, :, None], (dreward_block / counts[:, None])[:, None, :], 0.0).reshape(RESP_DEV * SEQ, HEADS)
        head_acc = head_acc + jnp.dot(normed.T, dscore, precision=lax.Precision.HIGHEST)
        dnormed = jnp.dot(dscore, heads32.T, precision=lax.Precision.HIGHEST)
        gain_acc = gain_acc + lax.optimization_barrier(jnp.sum(dnormed * hidden * rinv[:, None], axis=0))
        inner = lax.optimization_barrier(jnp.sum(hidden * gain32[None, :] * dnormed, axis=1))
        dhidden = (rinv[:, None] * gain32[None, :] * dnormed - hidden * (rinv ** 3 * inner / D)[:, None]).astype(jnp.bfloat16)
        proj_acc = proj_acc + jnp.dot(dhidden.T, attn_block, preferred_element_type=jnp.float32)
        return ((proj_acc, head_acc, gain_acc), None)
    start = (jnp.zeros((D, HIN), jnp.float32), jnp.zeros((D, HEADS), jnp.float32), jnp.zeros((D,), jnp.float32))
    (proj_grad, head_grad, gain_grad), unused = lax.scan(second_pass, start, (attn_blocks, resid_blocks, length_blocks, dreward))
    return (uwo, proj_grad, head_grad, gain_grad)
```

```python
import jax
import jax.numpy as jnp
from jax import lax
from jax.sharding import PartitionSpec as P


EPS_NORM = 1e-06
EPS_VAR = 1e-05
PENALTY = 0.5
LINE_LIMIT = 4


def swap(value, bit, axis="tensor"):
    return lax.ppermute(value, axis, [(i, i ^ bit) for i in range(lax.axis_size(axis))])


def gather_rows(own):
    n_dp = lax.axis_size("dp")
    line = n_dp // 2
    if line > LINE_LIMIT:
        return lax.all_gather(own, "dp", axis=0)
    d = lax.axis_index("dp")
    z, x = d // 2, d % 2

    def pair(value, first, last):
        return lax.ppermute(
            value, "dp", [(i, i ^ 1) for i in range(n_dp) if first <= i // 2 <= last]
        )

    found = jnp.zeros((n_dp,) + own.shape, own.dtype)
    found = lax.dynamic_update_index_in_dim(found, own, d, 0)
    found = lax.dynamic_update_index_in_dim(found, pair(own, 0, line - 1), d ^ 1, 0)
    up, down = own, own
    ups, downs = {}, {}
    for s in range(1, line):
        up = lax.ppermute(up, "dp", [(i, i + 2) for i in range(2 * (s - 1), n_dp - 2)])
        down = lax.ppermute(down, "dp", [(i, i - 2) for i in range(2, n_dp - 2 * (s - 1))])
        ups[s] = (up, pair(up, s, line - 1))
        downs[s] = (down, pair(down, 0, line - 1 - s))
    for s in range(1, line):
        place = 2 * ((z - s) % line)
        mine = ups[s][0] + downs[line - s][0]
        twin = ups[s][1] + downs[line - s][1]
        found = lax.dynamic_update_index_in_dim(found, mine, place + x, 0)
        found = lax.dynamic_update_index_in_dim(found, twin, place + 1 - x, 0)
    return found


def per_device(attn_out, resid, out_proj, heads, gain, lengths):
    f32, bf16 = jnp.float32, jnp.bfloat16
    rows, width = attn_out.shape
    cols = resid.shape[1]
    resp_dev = lengths.shape[0]
    seq_len = rows // resp_dev
    members = heads.shape[1]
    n_t = lax.axis_size("tensor")
    n_dp = lax.axis_size("dp")
    model = cols * n_t
    block = model // n_dp
    quarter = rows // n_t
    resp = resp_dev // n_t
    t = lax.axis_index("tensor")
    d = lax.axis_index("dp")
    low, high = t % 2, t // 2
    highest = lax.Precision.HIGHEST

    def pick(value, at, axis):
        return lax.dynamic_index_in_dim(value, at, axis, keepdims=False)

    gain_heads = jnp.concatenate([heads.astype(f32).T, gain.astype(f32)[None]], 0)
    bits = [1 << i for i in range((n_t - 1).bit_length())]
    parts = gain_heads[None]
    for bit in bits:
        parts = jnp.concatenate([parts, swap(parts, bit)], 0)
    order = [0]
    for bit in bits:
        order = order + [i ^ bit for i in order]
    where_is = jnp.array(order, jnp.int32)
    everything = jnp.concatenate([pick(parts, where_is[t ^ j], 0) for j in range(n_t)], 1)
    heads_all, gain_all = everything[:members], everything[members]

    attn_all = gather_rows(attn_out)

    a4 = attn_out.reshape(n_t // 2, 2, quarter, width)
    r4 = resid.reshape(n_t // 2, 2, quarter, cols)
    half = rows // 2
    a_keep, a_send = (pick(a4, b, 1).reshape(half, width) for b in (low, 1 - low))
    r_keep, r_send = (pick(r4, b, 1).reshape(half, cols) for b in (low, 1 - low))
    pieces = []
    for j in range(n_t):
        w = out_proj[:, j * cols:(j + 1) * cols]
        own = (t == j).astype(f32)
        send = jnp.dot(a_send, w, preferred_element_type=f32) + own * r_send.astype(f32)
        got = swap(send.astype(bf16), 1)
        keep = jnp.dot(a_keep, w, preferred_element_type=f32) + own * r_keep.astype(f32)
        pair = (keep + got.astype(f32)).reshape(n_t // 2, quarter, cols)
        got = swap(pick(pair, 1 - high, 0).astype(bf16), 2)
        pieces.append(pick(pair, high, 0) + got.astype(f32))
    hidden = jnp.concatenate(pieces, 1)
    full = hidden.astype(bf16).reshape(quarter, n_dp, block).transpose(1, 0, 2)
    moved = lax.all_to_all(full, "dp", 0, 0, tiled=True)
    arrived = {0: moved}
    arrived[2] = swap(moved, 2)
    arrived[1] = swap(moved, 1)
    arrived[3] = swap(arrived[2], 1)

    squares = jnp.sum(hidden * hidden, axis=1)
    raw = lax.dot_general(
        heads_all * gain_all[None, :], hidden, (((1,), (1,)), ((), ())), precision=highest
    )
    rinv = lax.rsqrt(squares / model + EPS_NORM)
    scores = raw * rinv[None, :]
    length = lax.dynamic_slice_in_dim(lengths, t * resp, resp)
    position = lax.broadcasted_iota(jnp.int32, (resp, seq_len), 1)
    inside = position <= length[:, None]
    counts = (length + 1).astype(f32)
    per_resp = scores.reshape(members, resp, seq_len)
    rewards = jnp.sum(jnp.where(inside[None], per_resp, 0.0), axis=2) / counts[None, :]
    pairs = rewards.reshape(members, resp // 2, 2)
    weight = jax.nn.sigmoid(pairs[:, :, 1] - pairs[:, :, 0])
    dreward = jnp.stack([-weight, weight], axis=2).reshape(members, resp)
    dscore = jnp.where(inside[None], (dreward / counts[None, :])[:, :, None], 0.0).reshape(
        members, quarter
    )
    inner = jnp.sum(dscore * raw, axis=0)
    coef = rinv**3 * inner / model
    lead = dscore * rinv[None, :]
    h_term = jnp.dot(lead, hidden, precision=highest)

    spread_rewards = jnp.pad(rewards, ((0, 0), (0, quarter - resp)))
    small = jnp.concatenate([lead, spread_rewards, coef[None]], 0)[None]
    for bit in bits:
        small = jnp.concatenate([small, swap(small, bit)], 0)
    t_index = jnp.array(order, jnp.int32)
    small = jnp.stack([pick(small, t_index[t ^ j], 0) for j in range(n_t)], 0)[None]
    dp_bits = [1 << i for i in range((n_dp - 1).bit_length())]
    dp_order = [0]
    for bit in dp_bits:
        small = jnp.concatenate([small, swap(small, bit, "dp")], 0)
        dp_order = dp_order + [i ^ bit for i in dp_order]
    dp_index = jnp.array(dp_order, jnp.int32)
    small = jnp.take(small, dp_index[jnp.arange(n_dp) ^ d], axis=0)
    lead_all = small[:, :, :members]
    rewards_all = small[:, :, members:2 * members, :resp]
    coef_all = small[:, :, 2 * members]

    h_sum = h_term.reshape(members, n_t // 2, 2, cols)
    h_sum = pick(h_sum, low, 2) + swap(pick(h_sum, 1 - low, 2), 1)
    h_sum = pick(h_sum, high, 1) + swap(pick(h_sum, 1 - high, 1), 2)
    for bit in dp_bits:
        h_sum = h_sum + swap(h_sum, bit, "dp")
    head_grad = (gain.astype(f32)[None, :] * h_sum).T
    gain_grad = jnp.sum(heads.astype(f32).T * h_sum, axis=0)

    center = jnp.mean(rewards_all, axis=(0, 1, 3))
    spread = jnp.mean((rewards_all - center[None, None, :, None]) ** 2, axis=(0, 1, 3))
    own_rewards = pick(rewards_all, d, 0)
    zed = (own_rewards - center[None, :, None]) * lax.rsqrt(spread + EPS_VAR)[None, :, None]
    zmean = jnp.mean(zed, axis=1)
    uwo = zmean - PENALTY * jnp.mean((zed - zmean[:, None, :]) ** 2, axis=1)
    uwo = uwo.reshape(resp_dev)

    lead_all = lead_all.transpose(2, 0, 1, 3).reshape(members, n_dp * rows)
    lead_hi = lead_all.astype(bf16)
    lead_lo = (lead_all - lead_hi.astype(f32)).astype(bf16)
    m2 = jnp.dot(
        jnp.concatenate([lead_hi, lead_lo], 0),
        attn_all.reshape(n_dp * rows, width),
        preferred_element_type=f32,
    )
    m = m2[:members] + m2[members:]
    gh_mine = lax.dynamic_slice_in_dim(heads_all * gain_all[None, :], d * block, block, 1)
    total = lax.dot_general(gh_mine, m, (((0,), (0,)), ((), ())), precision=highest)
    attn5 = attn_all.reshape(n_dp, n_t, quarter, width)
    for away in (0, 2, 1, 3):
        other = pick(attn5, t ^ away, 1).astype(f32) * pick(coef_all, t ^ away, 1)[:, :, None]
        total = total - lax.dot_general(
            arrived[away].reshape(n_dp * quarter, block),
            other.astype(bf16).reshape(n_dp * quarter, width),
            (((0,), (0,)), ((), ())),
            preferred_element_type=f32,
        )
    return (uwo, total, head_grad, gain_grad)


def solution(mesh):
    return jax.shard_map(
        per_device,
        mesh=mesh,
        in_specs=(
            P("dp", "tensor"),
            P("dp", "tensor"),
            P("tensor", None),
            P("tensor", None),
            P("tensor"),
            P("dp"),
        ),
        out_specs=(P("dp"), P("dp", "tensor"), P("tensor", None), P("tensor")),
        check_vma=False,
    )
```

```python
import jax
import jax.numpy as jnp
from jax import lax
from jax.sharding import PartitionSpec as P


EPS_NORM = 1e-06
EPS_VAR = 1e-05
PENALTY = 0.5
LINE_LIMIT = 4


def swap(value, bit, axis="tensor"):
    return lax.ppermute(value, axis, [(i, i ^ bit) for i in range(lax.axis_size(axis))])


def gather_rows(own):
    n_dp = lax.axis_size("dp")
    line = n_dp // 2
    if line > LINE_LIMIT:
        return lax.all_gather(own, "dp", axis=0)
    d = lax.axis_index("dp")
    z, x = d // 2, d % 2

    def pair(value, first, last):
        return lax.ppermute(
            value, "dp", [(i, i ^ 1) for i in range(n_dp) if first <= i // 2 <= last]
        )

    found = jnp.zeros((n_dp,) + own.shape, own.dtype)
    found = lax.dynamic_update_index_in_dim(found, own, d, 0)
    found = lax.dynamic_update_index_in_dim(found, pair(own, 0, line - 1), d ^ 1, 0)
    up, down = own, own
    ups, downs = {}, {}
    for s in range(1, line):
        up = lax.ppermute(up, "dp", [(i, i + 2) for i in range(2 * (s - 1), n_dp - 2)])
        down = lax.ppermute(down, "dp", [(i, i - 2) for i in range(2, n_dp - 2 * (s - 1))])
        ups[s] = (up, pair(up, s, line - 1))
        downs[s] = (down, pair(down, 0, line - 1 - s))
    for s in range(1, line):
        place = 2 * ((z - s) % line)
        mine = ups[s][0] + downs[line - s][0]
        twin = ups[s][1] + downs[line - s][1]
        found = lax.dynamic_update_index_in_dim(found, mine, place + x, 0)
        found = lax.dynamic_update_index_in_dim(found, twin, place + 1 - x, 0)
    return found


def per_device(attn_out, resid, out_proj, heads, gain, lengths):
    f32, bf16 = jnp.float32, jnp.bfloat16
    rows, width = attn_out.shape
    cols = resid.shape[1]
    resp_dev = lengths.shape[0]
    seq_len = rows // resp_dev
    members = heads.shape[1]
    n_t = lax.axis_size("tensor")
    n_dp = lax.axis_size("dp")
    model = cols * n_t
    block = model // n_dp
    quarter = rows // n_t
    resp = resp_dev // n_t
    t = lax.axis_index("tensor")
    d = lax.axis_index("dp")
    low, high = t % 2, t // 2
    highest = lax.Precision.HIGHEST

    def pick(value, at, axis):
        return lax.dynamic_index_in_dim(value, at, axis, keepdims=False)

    gain_heads = jnp.concatenate([heads.astype(f32).T, gain.astype(f32)[None]], 0)
    bits = [1 << i for i in range((n_t - 1).bit_length())]
    parts = gain_heads[None]
    for bit in bits:
        parts = jnp.concatenate([parts, swap(parts, bit)], 0)
    order = [0]
    for bit in bits:
        order = order + [i ^ bit for i in order]
    where_is = jnp.array(order, jnp.int32)
    everything = jnp.concatenate([pick(parts, where_is[t ^ j], 0) for j in range(n_t)], 1)
    heads_all, gain_all = everything[:members], everything[members]

    attn_all = gather_rows(attn_out)

    a4 = attn_out.reshape(n_t // 2, 2, quarter, width)
    r4 = resid.reshape(n_t // 2, 2, quarter, cols)
    half = rows // 2
    a_keep, a_send = (pick(a4, b, 1).reshape(half, width) for b in (low, 1 - low))
    r_keep, r_send = (pick(r4, b, 1).reshape(half, cols) for b in (low, 1 - low))
    pieces = []
    for j in range(n_t):
        w = out_proj[:, j * cols:(j + 1) * cols]
        own = (t == j).astype(f32)
        send = jnp.dot(a_send, w, preferred_element_type=f32) + own * r_send.astype(f32)
        got = swap(send.astype(bf16), 1)
        keep = jnp.dot(a_keep, w, preferred_element_type=f32) + own * r_keep.astype(f32)
        pair = (keep + got.astype(f32)).reshape(n_t // 2, quarter, cols)
        got = swap(pick(pair, 1 - high, 0).astype(bf16), 2)
        pieces.append(pick(pair, high, 0) + got.astype(f32))
    hidden = jnp.concatenate(pieces, 1)
    full = jnp.concatenate(
        [
            piece.astype(bf16).reshape(quarter, cols // block, block).transpose(1, 0, 2)
            for piece in pieces
        ],
        0,
    )
    moved = lax.all_to_all(full, "dp", 0, 0, tiled=True)
    arrived = {0: moved}
    arrived[2] = swap(moved, 2)
    arrived[1] = swap(moved, 1)
    arrived[3] = swap(arrived[2], 1)

    squares = jnp.sum(hidden * hidden, axis=1)
    raw = lax.dot_general(
        heads_all * gain_all[None, :], hidden, (((1,), (1,)), ((), ())), precision=highest
    )
    rinv = lax.rsqrt(squares / model + EPS_NORM)
    scores = raw * rinv[None, :]
    length = lax.dynamic_slice_in_dim(lengths, t * resp, resp)
    position = lax.broadcasted_iota(jnp.int32, (resp, seq_len), 1)
    inside = position <= length[:, None]
    counts = (length + 1).astype(f32)
    per_resp = scores.reshape(members, resp, seq_len)
    rewards = jnp.sum(jnp.where(inside[None], per_resp, 0.0), axis=2) / counts[None, :]
    pairs = rewards.reshape(members, resp // 2, 2)
    weight = jax.nn.sigmoid(pairs[:, :, 1] - pairs[:, :, 0])
    dreward = jnp.stack([-weight, weight], axis=2).reshape(members, resp)
    dscore = jnp.where(inside[None], (dreward / counts[None, :])[:, :, None], 0.0).reshape(
        members, quarter
    )
    inner = jnp.sum(dscore * raw, axis=0)
    coef = rinv**3 * inner / model
    lead = dscore * rinv[None, :]
    h_term = jnp.dot(lead, hidden, precision=highest)

    spread_rewards = jnp.pad(rewards, ((0, 0), (0, quarter - resp)))
    small = jnp.concatenate([lead, spread_rewards, coef[None]], 0)[None]
    for bit in bits:
        small = jnp.concatenate([small, swap(small, bit)], 0)
    t_index = jnp.array(order, jnp.int32)
    small = jnp.stack([pick(small, t_index[t ^ j], 0) for j in range(n_t)], 0)[None]
    dp_bits = [1 << i for i in range((n_dp - 1).bit_length())]
    dp_order = [0]
    for bit in dp_bits:
        small = jnp.concatenate([small, swap(small, bit, "dp")], 0)
        dp_order = dp_order + [i ^ bit for i in dp_order]
    dp_index = jnp.array(dp_order, jnp.int32)
    small = jnp.take(small, dp_index[jnp.arange(n_dp) ^ d], axis=0)
    lead_all = small[:, :, :members]
    rewards_all = small[:, :, members:2 * members, :resp]
    coef_all = small[:, :, 2 * members]

    h_sum = h_term.reshape(members, n_t // 2, 2, cols)
    h_sum = pick(h_sum, low, 2) + swap(pick(h_sum, 1 - low, 2), 1)
    h_sum = pick(h_sum, high, 1) + swap(pick(h_sum, 1 - high, 1), 2)
    for bit in dp_bits:
        h_sum = h_sum + swap(h_sum, bit, "dp")
    head_grad = (gain.astype(f32)[None, :] * h_sum).T
    gain_grad = jnp.sum(heads.astype(f32).T * h_sum, axis=0)

    center = jnp.mean(rewards_all, axis=(0, 1, 3))
    spread = jnp.mean((rewards_all - center[None, None, :, None]) ** 2, axis=(0, 1, 3))
    own_rewards = pick(rewards_all, d, 0)
    zed = (own_rewards - center[None, :, None]) * lax.rsqrt(spread + EPS_VAR)[None, :, None]
    zmean = jnp.mean(zed, axis=1)
    uwo = zmean - PENALTY * jnp.mean((zed - zmean[:, None, :]) ** 2, axis=1)
    uwo = uwo.reshape(resp_dev)

    lead_all = lead_all.transpose(2, 0, 1, 3).reshape(members, n_dp * rows)
    lead_hi = lead_all.astype(bf16)
    lead_lo = (lead_all - lead_hi.astype(f32)).astype(bf16)
    m2 = jnp.dot(
        jnp.concatenate([lead_hi, lead_lo], 0),
        attn_all.reshape(n_dp * rows, width),
        preferred_element_type=f32,
    )
    m = m2[:members] + m2[members:]
    gh_mine = lax.dynamic_slice_in_dim(heads_all * gain_all[None, :], d * block, block, 1)
    total = lax.dot_general(gh_mine, m, (((0,), (0,)), ((), ())), precision=highest)
    attn5 = attn_all.reshape(n_dp, n_t, quarter, width)
    for away in (0, 2, 1, 3):
        other = pick(attn5, t ^ away, 1).astype(f32) * pick(coef_all, t ^ away, 1)[:, :, None]
        total = total - lax.dot_general(
            arrived[away].reshape(n_dp * quarter, block),
            other.astype(bf16).reshape(n_dp * quarter, width),
            (((0,), (0,)), ((), ())),
            preferred_element_type=f32,
        )
    return (uwo, total, head_grad, gain_grad)


def solution(mesh):
    return jax.shard_map(
        per_device,
        mesh=mesh,
        in_specs=(
            P("dp", "tensor"),
            P("dp", "tensor"),
            P("tensor", None),
            P("tensor", None),
            P("tensor"),
            P("dp"),
        ),
        out_specs=(P("dp"), P("dp", "tensor"), P("tensor", None), P("tensor")),
        check_vma=False,
    )
```
